128 devices in a mesh: row: 4 (over x_hi, core), col: 32 (over y, z, x_lo).
Axes of the slice: x: 4 (x_hi: 2, x_lo: 2; x = x_hi * 2 + x_lo), y: 4, z: 4, core: 2. Of those that a mesh axis runs over, the one named last changes fastest.
Arguments:
- panel: bfloat16 [3072, 98304], P('row', 'col'), may hold values from -0.01953125 to 0.01953125
- surface: bfloat16 [98304, 1024], P('col'), may hold values from -6 to 6
- flexibility: float32 [4, 768, 768], P('row'), may hold values from -0.21875 to 0.21875
- owner_map: int32 [24], replicated, may hold values from 0 to 23, each once
- adjacency: int32 [4, 2], P('row'), may hold values from 0 to 3, as said below
- live_rows: int32 [24], replicated, may hold values from 1 to 128, 2304 in all
Outputs:
- response: float32 [1024, 98304], P('row', 'col')
The draws below stay inside these ranges and needn't reach their ends.
Inputs may be any that keep to these rules, and one draw needn't show every extreme that they name: `adjacency`: each substructure lists 2 different neighbours, never itself. `owner_map`: every slot receives exactly one mortar block. `live_rows`: the live rows add up to 2304 and some block is full.
All inputs are finite; a program needn't handle non-finite values.
Results may differ from the reference program's by a relative error of at most 0.0029.
Values may be sent and summed in bfloat16 or wider, within the bound.
No kernel may reach another device: no remote copies, remote signals or barrier semaphores. Data moves between devices by JAX's collectives and lax.ppermute only.
A program may use at most 128 MiB of HBM per device.

```python
import math
import jax
import jax.numpy as jnp
import numpy as np
from jax import lax

ORDER = 768
MBLK = 128
NC = 98304
L = 1024
ITERS = 2
DEG = 2
NSUB = 4
M = 3072
NBLK = 24
N_ROW = 4


def draw_adjacency(key, part):
    first_key, second_key = jax.random.split(jax.random.fold_in(key, 11))
    first_step = jax.random.randint(first_key, (NSUB,), 1, NSUB)
    second_step = jax.random.randint(second_key, (NSUB,), 1, NSUB - 1)
    second_step = jnp.where(second_step >= first_step, second_step + 1, second_step)
    own_index = jnp.arange(NSUB, dtype=jnp.int32)
    return jnp.stack([(own_index + first_step) % NSUB, (own_index + second_step) % NSUB], axis=1).astype(jnp.int32)


def block_scale(stream_key, shape, pieces, low, high):
    factor_of, own = 1.0, jax.random.fold_in(stream_key, 6)
    for axis_at, blocks in pieces:
        heights = jnp.exp(jax.random.uniform(jax.random.fold_in(own, axis_at), (blocks,), jnp.float32, low / len(pieces), high / len(pieces)))
        factor_of = factor_of * jnp.repeat(heights, shape[axis_at] // blocks).reshape([-1 if axis == axis_at else 1 for axis in range(len(shape))])
    return factor_of


def split_up(number_of, total, reach, slope):
    portions = [(1 << 20) // math.isqrt(rank ** slope) + 1 for rank in range(2, number_of + 1)]
    rest, given = total - reach - (number_of - 1), [1] * (number_of - 1)
    while rest > 0:
        movable = [i for i in range(number_of - 1) if given[i] < reach]
        mass, remaining = sum([portions[i] for i in movable]), rest
        for i in movable:
            more = min(reach - given[i], max(1, remaining * portions[i] // mass), rest)
            given[i] = given[i] + more
            rest = rest - more
    return np.array([reach] + given)


def ragged(key, number_of, total, most, slope):
    if number_of == 2:
        one = jax.random.randint(key, (), max(1, total - most), min(most, total - 1) + 1)
        return jnp.stack([one, total - one])
    lengths = jnp.asarray(split_up(number_of, total, most, slope), jnp.int32)
    pairs = (number_of - 1) // 2
    donor, taker = lengths[1:1 + 2 * pairs:2], lengths[2:2 + 2 * pairs:2]
    room = jnp.minimum(donor - 1, most - taker)
    shifted = jax.random.randint(jax.random.fold_in(key, 1), (pairs,), 0, 1 << 20) % (room + 1)
    lengths = lengths.at[1:1 + 2 * pairs:2].set(donor - shifted).at[2:2 + 2 * pairs:2].set(taker + shifted)
    return lengths[jax.random.permutation(jax.random.fold_in(key, 2), number_of)]


def gaussian(rng, extent, width, bound, pieces=(), kind=jnp.bfloat16):
    drawn = width * jax.random.normal(rng, extent, jnp.float32)
    if pieces:
        drawn = drawn * block_scale(rng, extent, pieces, -0.22, 0.18)
    return jnp.clip(drawn, -bound, bound).astype(kind)


def setup_inputs(seed: int = 0) -> dict:
    splits = jax.random.split(jax.random.key(seed), 7)
    panel = gaussian(splits[0], (M, NC), NC ** -0.5, 0.01953125, ((0, 4), (1, 32)))
    surface = gaussian(splits[1], (NC, L), 1.0, 6.0, ((0, 32),))
    flexibility = gaussian(splits[2], (NSUB, ORDER, ORDER), ORDER ** -0.5, 0.21875, ((0, 4),), jnp.float32)
    owner_map = jax.random.permutation(splits[3], NBLK).astype(jnp.int32)
    adjacency = draw_adjacency(jax.random.fold_in(splits[6], 71), 0)
    live_rows = ragged(splits[5], NBLK, NBLK * 3 * MBLK // 4, MBLK, 2).astype(jnp.int32)
    return dict(panel=panel, surface=surface, flexibility=flexibility, owner_map=owner_map, adjacency=adjacency, live_rows=live_rows)


DAMPING = 0.6
COUPLING = 0.5

def live_pattern(live_rows):
    offsets = jnp.arange(MBLK, dtype=jnp.int32)
    return (offsets[None, :] < live_rows[:, None]).astype(jnp.float32)

def reference(panel, surface, flexibility, owner_map, adjacency, live_rows):
    traction = lax.dot_general(surface, panel, (((0,), (1,)), ((), ())), preferred_element_type=jnp.float32)
    pattern = live_pattern(live_rows)
    blocks = traction.reshape(L, NBLK, MBLK) * pattern[None]
    inverse = jnp.zeros((NBLK,), jnp.int32).at[owner_map].set(jnp.arange(NBLK, dtype=jnp.int32))
    load_blocks = jnp.take(blocks, inverse, axis=1).reshape(L, NSUB, ORDER)
    neighbour_matrix = jnp.zeros((NSUB, NSUB), jnp.float32)
    for column in range(DEG):
        hits = adjacency[:, column][:, None] == jnp.arange(NSUB, dtype=jnp.int32)[None, :]
        neighbour_matrix = neighbour_matrix + hits.astype(jnp.float32)
    traces = jnp.zeros((L, NSUB, ORDER), jnp.float32)
    for sweep_index in range(ITERS):
        coupled = load_blocks + COUPLING * jnp.einsum('sn,lno->lso', neighbour_matrix, traces, precision=lax.Precision.HIGHEST)
        applied = jnp.einsum('sij,lsj->lsi', flexibility, coupled, precision=lax.Precision.HIGHEST)
        traces = (1.0 - DAMPING) * traces + DAMPING * applied
    rounded = traces.astype(jnp.bfloat16).reshape(L, NBLK, MBLK)
    updated = (jnp.take(rounded, owner_map, axis=1) * pattern[None].astype(jnp.bfloat16)).reshape(L, M)
    gain_factor = math.sqrt(NC / M)
    running_total = jnp.zeros((L, NC), jnp.float32)
    for block_row in range(N_ROW):
        lower = block_row * ORDER
        row_term = gain_factor * jnp.dot(updated[:, lower:lower + ORDER], panel[lower:lower + ORDER, :], preferred_element_type=jnp.float32)
        running_total = running_total + row_term
    return running_total
```

```python
import math

import jax
import jax.numpy as jnp
from jax import lax
from jax.sharding import PartitionSpec as P

MBLK = 128
ITERS = 2
DAMPING = 0.6
COUPLING = 0.5
AXES = ("row", "col")
HEAD = 13.0
LOW = -100.0
PAD = 8


def swap(array, flip):
    rows = lax.axis_size("row")
    return lax.ppermute(array, "row", [(i, i ^ flip) for i in range(rows)])


def exponent_of(array):
    peak = jnp.max(jnp.abs(array))
    return jnp.clip(jnp.floor(jnp.log2(peak)), LOW, 100.0)


def from_everyone(array, axis):
    devices = lax.axis_size(axis)
    return lax.all_to_all(
        jnp.broadcast_to(array[None], (devices, *array.shape)), axis, 0, 0, tiled=True
    )


def body(panel, surface, flexibility, owner_map, adjacency, live_rows):
    order_rows, column_count = panel.shape
    row_total = lax.axis_size("row")
    col_total = lax.axis_size("col")
    own_row = lax.axis_index("row")
    load_total = surface.shape[1]
    block_count = order_rows // MBLK
    block_total = owner_map.shape[0]
    group = load_total // (row_total * col_total)

    panel_beside = swap(panel, 1)
    flex_own = flexibility[0]
    flex_exp = exponent_of(flex_own)
    extra = jnp.concatenate(
        [
            jnp.full((1,), flex_exp, jnp.float32),
            adjacency[0].astype(jnp.float32),
            jnp.zeros((PAD - 3,), jnp.float32),
        ]
    )
    flex_packed = jnp.concatenate(
        [
            (flex_own * jnp.exp2(HEAD - flex_exp)).astype(jnp.float16),
            jnp.broadcast_to(extra[:, None], (PAD, order_rows)).astype(jnp.float16),
        ],
        axis=0,
    )
    flex_far = swap(flex_packed, 2)
    flex_two = swap(jnp.stack([flex_packed, flex_far]), 1)

    def unpacked(packed):
        scale = jnp.exp2(packed[order_rows, 0].astype(jnp.float32) - HEAD)
        return packed[:order_rows].astype(jnp.float32) * scale

    flex_all = [flex_own, unpacked(flex_far), unpacked(flex_two[0]), unpacked(flex_two[1])]
    near_lists = jnp.stack(
        [
            adjacency[0],
            flex_far[order_rows + 1 : order_rows + 3, 0].astype(jnp.int32),
            flex_two[0, order_rows + 1 : order_rows + 3, 0].astype(jnp.int32),
            flex_two[1, order_rows + 1 : order_rows + 3, 0].astype(jnp.int32),
        ]
    )
    places = own_row ^ jnp.array([0, 2, 1, 3], jnp.int32)
    near = jnp.sum(
        (near_lists[:, :, None] == places[None, None, :]).astype(jnp.float32), axis=1
    )

    partial = lax.dot_general(
        surface, panel, (((0,), (1,)), ((), ())), preferred_element_type=jnp.float32
    )
    part_exp = exponent_of(partial)
    pieces = (partial * jnp.exp2(HEAD - part_exp)).astype(jnp.float16)
    pieces = pieces.reshape(row_total, col_total, group, block_count, MBLK)
    pieces = pieces.transpose(1, 0, 3, 2, 4)
    pieces = pieces.reshape(col_total, row_total * block_count * group, MBLK)
    tail = jnp.full((col_total, PAD, MBLK), part_exp, jnp.float32).astype(jnp.float16)
    received = lax.all_to_all(
        jnp.concatenate([pieces, tail], axis=1), "col", 0, 0, tiled=True
    )
    scales = jnp.exp2(received[:, -1, :].astype(jnp.float32) - HEAD)
    traction = jnp.sum(received[:, :-PAD].astype(jnp.float32) * scales[:, None, :], axis=0)

    own_far = own_row // 2
    own_core = own_row % 2
    traction = traction.reshape(2, 2, block_count, group, MBLK)
    kept = lax.dynamic_index_in_dim(traction, own_far, 0, keepdims=False)
    sent = lax.dynamic_index_in_dim(traction, 1 - own_far, 0, keepdims=False)
    both = jnp.stack([kept, swap(sent, 2)])
    kept = lax.dynamic_index_in_dim(both, own_core, 1, keepdims=False)
    sent = lax.dynamic_index_in_dim(both, 1 - own_core, 1, keepdims=False)
    every_block = jnp.stack([kept, swap(sent, 1)]).reshape(block_total, group, MBLK)

    slot_ids = (places[:, None] * block_count + jnp.arange(block_count, dtype=jnp.int32)).reshape(-1)
    blocks = jnp.arange(block_total, dtype=jnp.int32)
    inverse = jnp.sum(
        jnp.where(owner_map[None, :] == slot_ids[:, None], blocks[None, :], 0), axis=1
    )
    apart = (inverse // block_count) ^ own_row
    source = ((apart % 2) * 2 + apart // 2) * block_count + inverse % block_count
    offsets = jnp.arange(MBLK, dtype=jnp.int32)
    live = (offsets[None, :] < live_rows[:, None]).astype(jnp.float32)
    loads = jnp.take(every_block, source, axis=0) * jnp.take(live, inverse, axis=0)[:, None, :]
    loads = loads.reshape(row_total, block_count, group, MBLK).transpose(0, 2, 1, 3)
    loads = loads.reshape(row_total, group, order_rows)

    def apply_each(values):
        return jnp.stack(
            [
                lax.dot_general(
                    values[s],
                    flex_all[s],
                    (((1,), (1,)), ((), ())),
                    precision=lax.Precision.HIGH,
                    preferred_element_type=jnp.float32,
                )
                for s in range(row_total)
            ]
        )

    traces = DAMPING * apply_each(loads)
    for _ in range(ITERS - 1):
        around = sum(near[:, n, None, None] * traces[n][None] for n in range(row_total))
        traces = (1.0 - DAMPING) * traces + DAMPING * apply_each(loads + COUPLING * around)

    slots = traces.astype(jnp.bfloat16).reshape(row_total, group, block_count, MBLK)
    slots = slots.transpose(0, 2, 1, 3).reshape(block_total, group, MBLK)
    row_ids = slot_ids.reshape(row_total, block_count)

    def rows_of(first, second):
        ids = jnp.concatenate([row_ids[first], row_ids[second]])
        owners = jnp.take(owner_map, ids)
        apart = (owners // block_count) ^ own_row
        at = ((apart % 2) * 2 + apart // 2) * block_count + owners % block_count
        return jnp.take(slots, at, axis=0) * jnp.take(live, ids, axis=0)[:, None, :].astype(jnp.bfloat16)

    mine = rows_of(0, 2)
    theirs = swap(rows_of(1, 3), 2)
    every_load = from_everyone(jnp.stack([mine, theirs]), "col")
    every_load = every_load.transpose(1, 0, 3, 2, 4)
    every_load = every_load.reshape(2, col_total * group, 2 * order_rows)

    gain_factor = math.sqrt(column_count * col_total / (order_rows * row_total))

    def times_panel(values):
        return gain_factor * (
            jnp.dot(values[:, :order_rows], panel, preferred_element_type=jnp.float32)
            + jnp.dot(values[:, order_rows:], panel_beside, preferred_element_type=jnp.float32)
        )

    away = swap(times_panel(every_load[1]).astype(jnp.bfloat16), 2)
    return times_panel(every_load[0]) + away.astype(jnp.float32)


def solution(mesh):
    in_specs = (P("row", "col"), P("col", None), P("row", None, None), P(), P("row", None), P())
    out_specs = P("row", "col")
    return jax.shard_map(body, mesh=mesh, in_specs=in_specs, out_specs=out_specs, check_vma=False)
```

```python
import math

import jax
import jax.numpy as jnp
from jax import lax
from jax.experimental import pallas as pl
from jax.experimental.pallas import tpu as pltpu
from jax.sharding import PartitionSpec as P


MBLK = 128
ITERS = 2
DAMPING = 0.6
COUPLING = 0.5
PAD = 8
CHUNKS = 2
LISTED = 16.0
MIB = 1 << 20
PART_SCALE = 2048.0
FLEX_SCALE = 131072.0


def swap(array, flip):
    rows = lax.axis_size("row")
    return lax.ppermute(array, "row", [(i, i ^ flip) for i in range(rows)])


def far_swap(array, flip_row, flip_col):
    rows, cols = lax.axis_size("row"), lax.axis_size("col")
    pairs = [
        (r * cols + c, (r ^ flip_row) * cols + (c ^ flip_col)) for r in range(rows) for c in range(cols)
    ]
    return lax.ppermute(array, ("row", "col"), pairs)


def to_root(values, scale):
    return (scale * jnp.sign(values) * jnp.sqrt(jnp.abs(values))).astype(jnp.float16)


def from_root(roots, scale):
    roots = roots.astype(jnp.float32)
    return scale**-2 * (roots * jnp.abs(roots))


def split_in_two(values):
    high = lax.reduce_precision(values, 8, 7)
    return high.astype(jnp.bfloat16), (values - high).astype(jnp.bfloat16)


def planes():
    cols = lax.axis_size("col")
    return [list(range(low, cols, 2)) for low in range(2)]


def from_everyone(array, groups=None):
    devices = lax.axis_size("col") if groups is None else len(groups[0])
    return lax.all_to_all(
        jnp.broadcast_to(array[None], (devices, *array.shape)),
        "col",
        0,
        0,
        axis_index_groups=groups,
        tiled=True,
    )


def iterate(owner_ref, live_ref, me_ref, kept_ref, next_ref, far_ref, both_ref, *refs):
    stored = refs[0:8]
    here_ref, there_ref = refs[8:10]
    blocks_ref, loads_ref, slots_ref, inverse_ref, high_ref, low_ref, sems = refs[10:17]
    order = high_ref.shape[2]
    highs = [pltpu.make_async_copy(stored[i], high_ref.at[i], sems.at[i]) for i in range(4)]
    lows = [pltpu.make_async_copy(stored[4 + i], low_ref.at[i], sems.at[4 + i]) for i in range(4)]
    for s in range(4):
        highs[s].start()
        lows[s].start()
    half = kept_ref.shape[0]
    blocks_ref[:half] = kept_ref[...] + next_ref[...]
    blocks_ref[half:] = far_ref[...] + both_ref[...]
    me = me_ref[0]
    total = blocks_ref.shape[0]
    count = total // 4
    group = blocks_ref.shape[1]
    places = [me ^ flip for flip in range(4)]

    def place_of(block):
        return ((block // count) ^ me) * count + lax.rem(block, count)

    for b in range(total):
        inverse_ref[owner_ref[b]] = b
    lane = lax.broadcasted_iota(jnp.int32, (group, MBLK), 1)
    for s in range(4):
        for j in range(count):
            block = inverse_ref[places[s] * count + j]
            values = blocks_ref[place_of(block)]
            loads_ref[s, :, j * MBLK : (j + 1) * MBLK] = jnp.where(
                lane < live_ref[block], values, 0.0
            )

    def apply(values, s):
        high = values.astype(jnp.bfloat16)
        low = (values - high.astype(jnp.float32)).astype(jnp.bfloat16)
        dims = (((1,), (1,)), ((), ()))
        both = lax.dot_general(
            jnp.concatenate([high, low], axis=0),
            high_ref[s, :order],
            dims,
            preferred_element_type=jnp.float32,
        )
        rest = lax.dot_general(high, low_ref[s, :order], dims, preferred_element_type=jnp.float32)
        return both[:group] + both[group:] + rest

    traces = []
    for s in range(4):
        highs[s].wait()
        lows[s].wait()
        traces.append(DAMPING * apply(loads_ref[s], s))
    for _ in range(ITERS - 1):
        coupled = []
        for s in range(4):
            around = jnp.zeros_like(traces[0])
            for n in range(4):
                place = places[n].astype(jnp.float32)
                for k in range(2):
                    listed = high_ref[s, order + k * PAD : order + (k + 1) * PAD].astype(jnp.float32)
                    around = around + jnp.where(LISTED * listed == place, traces[n], 0.0)
            coupled.append(loads_ref[s] + COUPLING * around)
        traces = [
            (1.0 - DAMPING) * traces[s] + DAMPING * apply(coupled[s], s) for s in range(4)
        ]
    for s in range(4):
        for j in range(count):
            slots_ref[s * count + j] = traces[s][:, j * MBLK : (j + 1) * MBLK]
    for out_ref, pair in ((here_ref, (0, 1)), (there_ref, (2, 3))):
        for i, flip in enumerate(pair):
            for j in range(count):
                block = (me ^ flip) * count + j
                values = slots_ref[place_of(owner_ref[block])]
                values = jnp.where(lane < live_ref[block], values, 0.0).astype(jnp.bfloat16)
                if out_ref is there_ref:
                    out_ref[i * count + j] = values
                else:
                    for copy in range(out_ref.shape[0]):
                        out_ref[copy, i * count + j] = values


def body(panel, surface, flexibility, owner_map, adjacency, live_rows):
    order_rows, column_count = panel.shape
    row_total = lax.axis_size("row")
    col_total = lax.axis_size("col")
    own_row = lax.axis_index("row")
    load_total = surface.shape[1]
    block_count = order_rows // MBLK
    block_total = owner_map.shape[0]
    group = load_total // (row_total * col_total)

    flex_own = flexibility[0]
    lists = jnp.repeat(adjacency[0].astype(jnp.float32) / LISTED, PAD)
    flex_own = jnp.concatenate(
        [flex_own, jnp.broadcast_to(lists[:, None], (2 * PAD, order_rows))], axis=0
    )
    flex_packed = to_root(flex_own, FLEX_SCALE)
    flex_far = swap(flex_packed, 2)
    panel_beside = swap(panel, 1)
    surface, flex_packed, flex_own = lax.optimization_barrier((surface, flex_packed, flex_own))

    partial = lax.dot_general(
        surface, panel, (((0,), (1,)), ((), ())), preferred_element_type=jnp.float32
    )
    pieces = to_root(partial, PART_SCALE)
    pieces = pieces.reshape(row_total, col_total // 2, 2, group, block_count, MBLK)
    pieces = pieces.transpose(1, 2, 0, 4, 3, 5)
    pieces = pieces.reshape(col_total // 2, 2 * row_total * block_count * group, MBLK)
    received = lax.all_to_all(pieces, "col", 0, 0, axis_index_groups=planes(), tiled=True)
    received, panel_beside = lax.optimization_barrier((received, panel_beside))

    high, low = split_in_two(flex_own)
    far_high, far_low = split_in_two(from_root(flex_far, FLEX_SCALE))
    highs = [high, swap(high, 1), far_high, swap(far_high, 1)]
    lows = [low, swap(low, 1), far_low, swap(far_low, 1)]
    traction = jnp.sum(from_root(received, PART_SCALE), axis=0)

    own_far = own_row // 2
    own_core = own_row % 2
    own_low = lax.axis_index("col") % 2
    traction = traction.reshape(4, 2, block_count, group, MBLK)
    kept = lax.dynamic_index_in_dim(traction, own_core, 1, keepdims=False)
    sent = lax.dynamic_index_in_dim(traction, 1 - own_core, 1, keepdims=False)
    chip_rows = jnp.concatenate([kept, swap(sent, 1)], axis=1)

    def chip_part(low, far):
        return lax.dynamic_index_in_dim(chip_rows, low * 2 + far, 0, keepdims=False)

    from_far = far_swap(chip_part(own_low, own_far), 2, 0)
    from_next = far_swap(chip_part(1 - own_low, 1 - own_far), 0, 1)
    from_both = far_swap(chip_part(1 - own_low, own_far), 2, 1)

    smem = pl.BlockSpec(memory_space=pltpu.SMEM)
    vmem = pl.BlockSpec(memory_space=pltpu.VMEM)
    hbm = pl.BlockSpec(memory_space=pl.ANY)
    shape = (2 * block_count, group, MBLK)
    here, there = pl.pallas_call(
        iterate,
        out_shape=(
            jax.ShapeDtypeStruct((col_total, *shape), jnp.bfloat16),
            jax.ShapeDtypeStruct(shape, jnp.bfloat16),
        ),
        in_specs=[smem] * 3 + [vmem] * 4 + [hbm] * 8,
        out_specs=(vmem, vmem),
        scratch_shapes=[
            pltpu.VMEM((block_total, group, MBLK), jnp.float32),
            pltpu.VMEM((row_total, group, order_rows), jnp.float32),
            pltpu.VMEM((block_total, group, MBLK), jnp.float32),
            pltpu.SMEM((block_total,), jnp.int32),
            pltpu.VMEM((row_total, order_rows + 2 * PAD, order_rows), jnp.bfloat16),
            pltpu.VMEM((row_total, order_rows + 2 * PAD, order_rows), jnp.bfloat16),
            pltpu.SemaphoreType.DMA((8,)),
        ],
        cost_estimate=pl.CostEstimate(
            flops=2 * ITERS * row_total * group * order_rows**2 * 24,
            bytes_accessed=4 * row_total * order_rows**2,
            transcendentals=0,
        ),
        compiler_params=pltpu.CompilerParams(vmem_limit_bytes=20 * MIB),
        name="iterate",
    )(
        owner_map,
        live_rows,
        jnp.full((1,), own_row, jnp.int32),
        chip_part(own_low, 1 - own_far),
        from_next,
        from_far,
        from_both,
        *highs,
        *lows,
    )

    gain_factor = math.sqrt(column_count * col_total / (order_rows * row_total))

    def as_rows(everyones):
        values = everyones.reshape(col_total, 2 * block_count, group, MBLK).transpose(0, 2, 1, 3)
        return values.reshape(col_total * group, 2 * order_rows)

    width = column_count // CHUNKS
    cuts = [slice(i * width, (i + 1) * width) for i in range(CHUNKS)]

    def times_panel(values, cut):
        return gain_factor * (
            jnp.dot(values[:, :order_rows], panel[:, cut], preferred_element_type=jnp.float32)
            + jnp.dot(
                values[:, order_rows:], panel_beside[:, cut], preferred_element_type=jnp.float32
            )
        )

    lent_rows = as_rows(lax.all_to_all(here, "col", 0, 0, tiled=True))
    home, beyond = far_swap(there, 2, 0), far_swap(there, 2, 1)
    home = jnp.where(own_low == 0, jnp.stack([home, beyond]), jnp.stack([beyond, home]))
    away = []
    for cut in cuts:
        lent = times_panel(lent_rows, cut).astype(jnp.bfloat16)
        lent, lent_rows = lax.optimization_barrier((lent, lent_rows))
        away.append(swap(lent, 2))
    home_rows = as_rows(from_everyone(home, planes()))
    own = lax.optimization_barrier([times_panel(home_rows, cut) for cut in cuts])
    return jnp.concatenate([o + a.astype(jnp.float32) for o, a in zip(own, away)], axis=1)


def solution(mesh):
    in_specs = (P("row", "col"), P("col", None), P("row", None, None), P(), P("row", None), P())
    out_specs = P("row", "col")
    return jax.shard_map(body, mesh=mesh, in_specs=in_specs, out_specs=out_specs, check_vma=False)
```

```python
import math

import jax
import jax.numpy as jnp
from jax import lax
from jax.experimental import pallas as pl
from jax.experimental.pallas import tpu as pltpu
from jax.sharding import PartitionSpec as P


MBLK = 128
ITERS = 2
DAMPING = 0.6
COUPLING = 0.5
PAD = 8
FIRST = 3
LISTED = 16.0
MIB = 1 << 20
PART_SCALE = 2048.0


def swap(array, flip):
    rows = lax.axis_size("row")
    return lax.ppermute(array, "row", [(i, i ^ flip) for i in range(rows)])


def far_swap(array, flip_row, flip_col):
    rows, cols = lax.axis_size("row"), lax.axis_size("col")
    pairs = [
        (r * cols + c, (r ^ flip_row) * cols + (c ^ flip_col)) for r in range(rows) for c in range(cols)
    ]
    return lax.ppermute(array, ("row", "col"), pairs)


def to_root(values, scale):
    return (scale * jnp.sign(values) * jnp.sqrt(jnp.abs(values))).astype(jnp.float16)


def from_root(roots, scale):
    roots = roots.astype(jnp.float32)
    return scale**-2 * (roots * jnp.abs(roots))


def split_in_two(values):
    high = lax.reduce_precision(values, 8, 7)
    return high.astype(jnp.bfloat16), (values - high).astype(jnp.bfloat16)


def planes():
    cols = lax.axis_size("col")
    return [list(range(low, cols, 2)) for low in range(2)]


def from_everyone(array, groups=None):
    devices = lax.axis_size("col") if groups is None else len(groups[0])
    return lax.all_to_all(
        jnp.broadcast_to(array[None], (devices, *array.shape)),
        "col",
        0,
        0,
        axis_index_groups=groups,
        tiled=True,
    )


def iterate(owner_ref, live_ref, me_ref, kept_ref, next_ref, far_ref, both_ref, *refs):
    stored = refs[0:8]
    here_ref, there_ref = refs[8:10]
    blocks_ref, loads_ref, slots_ref, inverse_ref, high_ref, low_ref, sems = refs[10:17]
    order = high_ref.shape[2]
    highs = [pltpu.make_async_copy(stored[i], high_ref.at[i], sems.at[i]) for i in range(4)]
    lows = [pltpu.make_async_copy(stored[4 + i], low_ref.at[i], sems.at[4 + i]) for i in range(4)]
    for s in range(4):
        highs[s].start()
        lows[s].start()
    half = kept_ref.shape[0]
    blocks_ref[:half] = kept_ref[...] + next_ref[...]
    blocks_ref[half:] = far_ref[...] + both_ref[...]
    me = me_ref[0]
    total = blocks_ref.shape[0]
    count = total // 4
    group = blocks_ref.shape[1]
    places = [me ^ flip for flip in range(4)]

    def place_of(block):
        row = sum((block >= k * count).astype(jnp.int32) for k in range(1, 4))
        return block + ((row ^ me) - row) * count

    for b in range(total):
        inverse_ref[owner_ref[b]] = b
    lane = lax.broadcasted_iota(jnp.int32, (group, MBLK), 1)
    for s in range(4):
        for j in range(count):
            block = inverse_ref[places[s] * count + j]
            values = blocks_ref[place_of(block)]
            loads_ref[s, :, j * MBLK : (j + 1) * MBLK] = jnp.where(
                lane < live_ref[block], values, 0.0
            )

    def apply(values, s):
        high = values.astype(jnp.bfloat16)
        low = (values - high.astype(jnp.float32)).astype(jnp.bfloat16)
        dims = (((1,), (1,)), ((), ()))
        both = lax.dot_general(
            jnp.concatenate([high, low], axis=0),
            high_ref[s, :order],
            dims,
            preferred_element_type=jnp.float32,
        )
        rest = lax.dot_general(high, low_ref[s, :order], dims, preferred_element_type=jnp.float32)
        return both[:group] + both[group:] + rest

    traces = []
    for s in range(4):
        highs[s].wait()
        lows[s].wait()
        traces.append(DAMPING * apply(loads_ref[s], s))
    for _ in range(ITERS - 1):
        coupled = []
        for s in range(4):
            around = jnp.zeros_like(traces[0])
            for n in range(4):
                place = places[n].astype(jnp.float32)
                for k in range(2):
                    listed = high_ref[s, order + k * PAD : order + (k + 1) * PAD].astype(jnp.float32)
                    around = around + jnp.where(LISTED * listed == place, traces[n], 0.0)
            coupled.append(loads_ref[s] + COUPLING * around)
        traces = [
            (1.0 - DAMPING) * traces[s] + DAMPING * apply(coupled[s], s) for s in range(4)
        ]
    for s in range(4):
        for j in range(count):
            slots_ref[s * count + j] = traces[s][:, j * MBLK : (j + 1) * MBLK]
    for out_ref, pair in ((here_ref, (0, 1)), (there_ref, (2, 3))):
        for i, flip in enumerate(pair):
            for j in range(count):
                block = (me ^ flip) * count + j
                values = slots_ref[place_of(owner_ref[block])]
                values = jnp.where(lane < live_ref[block], values, 0.0).astype(jnp.bfloat16)
                if out_ref is there_ref:
                    out_ref[i * count + j] = values
                else:
                    for copy in range(out_ref.shape[0]):
                        out_ref[copy, i * count + j] = values


def body(panel, surface, flexibility, owner_map, adjacency, live_rows):
    order_rows, column_count = panel.shape
    row_total = lax.axis_size("row")
    col_total = lax.axis_size("col")
    own_row = lax.axis_index("row")
    load_total = surface.shape[1]
    block_count = order_rows // MBLK
    block_total = owner_map.shape[0]
    group = load_total // (row_total * col_total)

    flex_own = flexibility[0]
    lists = jnp.repeat(adjacency[0].astype(jnp.float32) / LISTED, PAD)
    flex_own = jnp.concatenate(
        [flex_own, jnp.broadcast_to(lists[:, None], (2 * PAD, order_rows))], axis=0
    )
    flex_packed = (flex_own * 262144.0).astype(jnp.float16)
    flex_far = swap(flex_packed, 2)
    panel_beside = swap(panel, 1)
    surface, flex_packed, flex_own = lax.optimization_barrier((surface, flex_packed, flex_own))

    partial = lax.dot_general(
        surface, panel, (((0,), (1,)), ((), ())), preferred_element_type=jnp.float32
    )
    pieces = to_root(partial, PART_SCALE)
    pieces = pieces.reshape(row_total, col_total // 2, 2, group, block_count, MBLK)
    pieces = pieces.transpose(1, 2, 0, 4, 3, 5)
    pieces = pieces.reshape(col_total // 2, 2 * row_total * block_count * group, MBLK)
    received = lax.all_to_all(pieces, "col", 0, 0, axis_index_groups=planes(), tiled=True)

    high, low = split_in_two(flex_own)
    far_high, far_low = split_in_two((flex_far.astype(jnp.float32) / 262144.0))
    highs = [high, swap(high, 1), far_high, swap(far_high, 1)]
    lows = [low, swap(low, 1), far_low, swap(far_low, 1)]
    traction = jnp.sum(from_root(received, PART_SCALE), axis=0)
    traction, panel_beside = lax.optimization_barrier((traction, panel_beside))

    own_far = own_row // 2
    own_core = own_row % 2
    own_low = lax.axis_index("col") % 2
    traction = traction.reshape(4, 2, block_count, group, MBLK)
    kept = lax.dynamic_index_in_dim(traction, own_core, 1, keepdims=False)
    sent = lax.dynamic_index_in_dim(traction, 1 - own_core, 1, keepdims=False)
    chip_rows = jnp.concatenate([kept, swap(sent, 1)], axis=1)

    def chip_part(low, far):
        return lax.dynamic_index_in_dim(chip_rows, low * 2 + far, 0, keepdims=False)

    from_far = far_swap(chip_part(own_low, own_far), 2, 0)
    from_next = far_swap(chip_part(1 - own_low, 1 - own_far), 0, 1)
    from_both = far_swap(chip_part(1 - own_low, own_far), 2, 1)

    smem = pl.BlockSpec(memory_space=pltpu.SMEM)
    vmem = pl.BlockSpec(memory_space=pltpu.VMEM)
    hbm = pl.BlockSpec(memory_space=pl.ANY)
    shape = (2 * block_count, group, MBLK)
    here, there = pl.pallas_call(
        iterate,
        out_shape=(
            jax.ShapeDtypeStruct((col_total, *shape), jnp.bfloat16),
            jax.ShapeDtypeStruct(shape, jnp.bfloat16),
        ),
        in_specs=[smem] * 3 + [vmem] * 4 + [hbm] * 8,
        out_specs=(vmem, vmem),
        scratch_shapes=[
            pltpu.VMEM((block_total, group, MBLK), jnp.float32),
            pltpu.VMEM((row_total, group, order_rows), jnp.float32),
            pltpu.VMEM((block_total, group, MBLK), jnp.float32),
            pltpu.SMEM((block_total,), jnp.int32),
            pltpu.VMEM((row_total, order_rows + 2 * PAD, order_rows), jnp.bfloat16),
            pltpu.VMEM((row_total, order_rows + 2 * PAD, order_rows), jnp.bfloat16),
            pltpu.SemaphoreType.DMA((8,)),
        ],
        cost_estimate=pl.CostEstimate(
            flops=2 * ITERS * row_total * group * order_rows**2 * 24,
            bytes_accessed=4 * row_total * order_rows**2,
            transcendentals=0,
        ),
        compiler_params=pltpu.CompilerParams(vmem_limit_bytes=20 * MIB),
        name="iterate",
    )(
        owner_map,
        live_rows,
        jnp.full((1,), own_row, jnp.int32),
        chip_part(own_low, 1 - own_far),
        from_next,
        from_far,
        from_both,
        *highs,
        *lows,
    )

    gain_factor = math.sqrt(column_count * col_total / (order_rows * row_total))

    def as_rows(everyones):
        values = everyones.reshape(col_total, 2 * block_count, group, MBLK).transpose(0, 2, 1, 3)
        return values.reshape(col_total * group, 2 * order_rows)

    first = column_count // FIRST
    cuts = [slice(0, first), slice(first, column_count)]

    def times_panel(values, cut):
        return gain_factor * (
            jnp.dot(values[:, :order_rows], panel[:, cut], preferred_element_type=jnp.float32)
            + jnp.dot(
                values[:, order_rows:], panel_beside[:, cut], preferred_element_type=jnp.float32
            )
        )

    lent_rows = as_rows(lax.all_to_all(here, "col", 0, 0, tiled=True))
    home, beyond = far_swap(there, 2, 0), far_swap(there, 2, 1)
    home = jnp.where(own_low == 0, jnp.stack([home, beyond]), jnp.stack([beyond, home]))
    away = []
    for cut in cuts:
        lent = times_panel(lent_rows, cut).astype(jnp.bfloat16)
        lent, lent_rows = lax.optimization_barrier((lent, lent_rows))
        away.append(swap(lent, 2))
    home_rows = as_rows(from_everyone(home, planes()))
    own = lax.optimization_barrier([times_panel(home_rows, cut) for cut in cuts])
    return jnp.concatenate([o + a.astype(jnp.float32) for o, a in zip(own, away)], axis=1)


def solution(mesh):
    in_specs = (P("row", "col"), P("col", None), P("row", None, None), P(), P("row", None), P())
    out_specs = P("row", "col")
    return jax.shard_map(body, mesh=mesh, in_specs=in_specs, out_specs=out_specs, check_vma=False)
```
